32 devices in a mesh: expert: 8 (over z, y), helper: 4 (over x, core).
Axes of the slice: x: 2, y: 2, z: 4, core: 2. Of those that a mesh axis runs over, the one named last changes fastest.
Arguments:
- tokens: bfloat16 [32768, 768], P(('expert', 'helper')), may hold values from -6 to 6
- gate: float32 [32768], P(('expert', 'helper')), may hold values from 0.2 to 1
- expert_ids: int32 [32768, 1], P(('expert', 'helper')), may hold values from 0 to 31; in each aligned block of 1024 rows (0 to 1023, 1024 to 2047, ...) at most 48 rows name the same one
- backup_ids: int32 [32768, 1], P(('expert', 'helper')), may hold values from 0 to 31; in each aligned block of 1024 rows (0 to 1023, 1024 to 2047, ...) at most 48 rows name the same one
- capacity: int32 [32], replicated, may hold values from 2 to 48
- w_in: bfloat16 [32, 768, 3072], P('expert', None, 'helper'), may hold values from -0.21875 to 0.21875
- w_out: bfloat16 [32, 3072, 768], P('expert', 'helper'), may hold values from -0.109375 to 0.109375
Outputs:
- mixed: bfloat16 [32768, 768], P(('expert', 'helper'))
The draws below stay inside these ranges and needn't reach their ends.
Inputs may be any that keep to these rules, and one draw needn't show every extreme that they name: `expert_ids`: in the rows of one device no expert is the first expert of more than 48 rows; some expert reaches 48. `backup_ids`: in the rows of one device no expert is the backup of more than 48 rows; some expert reaches 48.
All inputs are finite; a program needn't handle non-finite values.
Results may differ from the reference program's by a relative error of at most 0.0095.
Values may be sent and summed in bfloat16 or wider, within the bound.
A program may use at most 192 MiB of HBM per device.

```python
import math
import jax
import jax.numpy as jnp
import numpy as np
from jax import lax

D = 768
FF = 3072
TOK_DEV = 1024
EXPERTS = 32
SLOT = 48
TOKENS = 32768
N_EXPERT = 8
N_HELPER = 4


def touch_ends(entries, stream_key, low, largest):
    place = [jax.random.randint(jax.random.fold_in(stream_key, axis), (), 0, length) for axis, length in enumerate(entries.shape)]
    longest = entries.shape.index(max(entries.shape))
    next_to = place[:longest] + [(place[longest] + 1) % entries.shape[longest]] + place[longest + 1:]
    return entries.at[tuple(place)].set(low).at[tuple(next_to)].set(largest)


def level_of(own_key, extent, pieces, smallest, high):
    def one(axis_at, blocks):
        steps = jax.random.uniform(jax.random.fold_in(jax.random.fold_in(own_key, 6), axis_at), (blocks,), jnp.float32, smallest / len(pieces), high / len(pieces))
        return jnp.repeat(jnp.exp(steps), extent[axis_at] // blocks).reshape((-1,) + (1,) * (len(extent) - axis_at - 1))

    loudness = one(*pieces[0])
    for cut in pieces[1:]:
        loudness = loudness * one(*cut)
    return loudness


def shared_out(stream_key, own, number, rows, count, top, reach, skew):
    sequence = jax.random.permutation(stream_key, count)
    crowded, ordinary = shares(count, rows * top, reach, skew, True), shares(count, rows * top, reach, skew, False)
    places = jnp.arange(count)

    def named(tallies, turn):
        used = int((tallies > 0).sum())
        fixed = max(1, used // 4)
        shifted = fixed + (places - fixed + turn * (used - fixed)) % max(1, count - fixed)
        return jnp.zeros((count,), jnp.int32).at[sequence[jnp.where(places < fixed, places, shifted)]].set(jnp.asarray(tallies, jnp.int32))

    tallies = jnp.where(number % 4 == 0, named(crowded, number // 4), named(ordinary, number - number // 4 - 1))
    mixed = jax.random.permutation(jax.random.fold_in(own, 3), count)
    giver, receiver = mixed[0:count // 2 * 2:2], mixed[1:count // 2 * 2:2]
    margin = jnp.minimum(tallies[giver] - 1, reach - tallies[receiver]) // 2
    margin = jnp.where((giver == sequence[0]) | (receiver == sequence[0]) | (tallies[receiver] == 0), 0, jnp.maximum(margin, 0))
    shifted = jax.random.randint(jax.random.fold_in(own, 4), (count // 2,), 0, 1 << 20) % (margin + 1)
    tallies = tallies.at[giver].add(-shifted).at[receiver].add(shifted)
    items = jnp.searchsorted(jnp.cumsum(tallies), jnp.arange(rows * top), side="right").astype(jnp.int32)
    listing = items.reshape(top, rows).T
    listing = listing[jax.random.permutation(jax.random.fold_in(own, 1), rows)]
    turn = jax.random.randint(jax.random.fold_in(own, 2), (rows, 1), 0, top)
    return jnp.take_along_axis(listing, (jnp.arange(top)[None, :] + turn) % top, axis=1)


def shares(amount, total, reach, lean, full):
    portions = [(1 << 20) // math.isqrt(rank ** lean) + 1 for rank in range(1, amount + 1)]
    largest = reach if full else min(reach, max(-(-total // amount), total * portions[0] // sum(portions)))
    least = 1 if total - largest >= amount - 1 else 0
    counts, surplus = [largest] + [least] * (amount - 1), total - largest - least * (amount - 1)
    while surplus > 0:
        free = [i for i in range(1, amount) if counts[i] < largest] or [i for i in range(1, amount) if counts[i] < reach]
        whole, budget = sum([portions[i] for i in free]), surplus
        for i in free:
            extra = min(reach - counts[i], max(1, budget * portions[i] // whole), surplus)
            counts[i] = counts[i] + extra
            surplus = surplus - extra
    return np.array(counts)


def centred(stream_key, shape, scale, most, pieces=(), kind=jnp.bfloat16):
    level = level_of(stream_key, shape, pieces, -0.22, 0.18) if pieces else 1.0
    values = jax.random.normal(stream_key, shape, jnp.float32) * scale * level
    return jnp.minimum(jnp.maximum(values, -most), most).astype(kind)


def setup_inputs(seed: int = 0) -> dict:
    arg_keys = jax.random.split(jax.random.key(seed), 8)
    tokens = centred(arg_keys[0], (TOKENS, D), 1.0, 6.0, ((0, 32),))
    gate = jnp.clip(0.2 + 0.8 * jax.random.uniform(arg_keys[1], (TOKENS,), jnp.float32) ** level_of(arg_keys[1], (TOKENS,), ((0, 32),), -0.2, 0.2), 0.2, 1.0)
    expert_ids_keys = jax.random.split(jax.random.fold_in(arg_keys[2], 1), TOKENS // TOK_DEV)
    expert_ids_turns = jax.random.permutation(jax.random.fold_in(arg_keys[2], 3), TOKENS // TOK_DEV)
    expert_ids = jax.vmap(lambda own, number: shared_out(jax.random.fold_in(arg_keys[2], 2), own, number, TOK_DEV, EXPERTS, 1, SLOT, 2))(expert_ids_keys, expert_ids_turns).reshape((TOKENS, 1))
    backup_ids_keys = jax.random.split(jax.random.fold_in(arg_keys[3], 1), TOKENS // TOK_DEV)
    backup_ids_turns = jax.random.permutation(jax.random.fold_in(arg_keys[3], 3), TOKENS // TOK_DEV)
    backup_ids = jax.vmap(lambda own, number: shared_out(jax.random.fold_in(arg_keys[3], 2), own, number, TOK_DEV, EXPERTS, 1, SLOT, 1))(backup_ids_keys, backup_ids_turns).reshape((TOKENS, 1))
    capacity = touch_ends(jax.random.randint(arg_keys[4], (EXPERTS,), 2, SLOT + 1), jax.random.fold_in(arg_keys[4], 1), 2, SLOT).astype(jnp.int32)
    w_in = centred(arg_keys[5], (EXPERTS, D, FF), D ** -0.5, 0.21875, ((0, 8), (2, 4)))
    w_out = centred(arg_keys[6], (EXPERTS, FF, D), FF ** -0.5, 0.109375, ((0, 8), (1, 4)))
    return dict(tokens=tokens, gate=gate, expert_ids=expert_ids, backup_ids=backup_ids, capacity=capacity, w_in=w_in, w_out=w_out)


def assign(first, backup, capacity, count, slot):
    columns = jnp.arange(count, dtype=jnp.int32)
    onehot = (first[:, None] == columns[None, :]).astype(jnp.int32)
    rank = jnp.sum((jnp.cumsum(onehot, axis=0) - onehot) * onehot, axis=1)
    limit = jnp.sum(onehot * capacity[None, :], axis=1)
    kept = rank < limit
    spill = (backup[:, None] == columns[None, :]).astype(jnp.int32) * (1 - kept.astype(jnp.int32))[:, None]
    spill_rank = jnp.sum((jnp.cumsum(spill, axis=0) - spill) * spill, axis=1)
    final = jnp.where(kept, first, backup).astype(jnp.int32)
    slots = jnp.where(kept, rank, slot + spill_rank).astype(jnp.int32)
    return slots, final


def expert_apply(rows, weight_in, weight_out):
    width = weight_in.shape[1] // N_HELPER
    total = jnp.zeros((rows.shape[0], rows.shape[1]), jnp.float32)
    for quarter in range(N_HELPER):
        inner = weight_in[:, quarter * width:(quarter + 1) * width].astype(jnp.float32)
        outer = weight_out[quarter * width:(quarter + 1) * width, :].astype(jnp.float32)
        hidden = jax.nn.relu(jnp.dot(rows.astype(jnp.float32), inner)).astype(jnp.bfloat16)
        part = jnp.dot(hidden.astype(jnp.float32), outer).astype(jnp.bfloat16)
        total = total + part.astype(jnp.float32)
    return total.astype(jnp.bfloat16)


def reference(tokens, gate, expert_ids, backup_ids, capacity, w_in, w_out):
    devices = N_EXPERT * N_HELPER
    room = 2 * SLOT
    first = expert_ids[:, 0].reshape(devices, TOK_DEV)
    backup = backup_ids[:, 0].reshape(devices, TOK_DEV)
    slots, final = jax.vmap(lambda a, b: assign(a, b, capacity, EXPERTS, SLOT))(first, backup)
    owner = jnp.arange(devices, dtype=jnp.int32)[:, None] * room + slots
    owner = owner.reshape(-1)
    final = final.reshape(-1)
    buffer = jnp.zeros((EXPERTS, devices * room, D), jnp.bfloat16).at[final, owner].set(tokens)
    results = lax.map(lambda item: expert_apply(item[0], item[1], item[2]), (buffer, w_in, w_out))
    picked = results[final, owner]
    return (gate[:, None] * picked.astype(jnp.float32)).astype(jnp.bfloat16)
```

```python
import functools

import jax
import jax.numpy as jnp
from jax import lax
from jax.experimental import pallas as pl
from jax.experimental.pallas import tpu as pltpu
from jax.sharding import PartitionSpec as P

MESH = pl.DeviceIdType.MESH
TILE = 16
CHUNK = 16
VMEM_BYTES = 60 * 2**20


def flip(index, mask):
    out, bit = index, 1
    while bit <= mask:
        if mask & bit:
            out = out + bit - 2 * bit * ((index // bit) % 2)
        bit *= 2
    return out


def visits(owners):
    masks = list(range(1, owners))
    return sorted(masks, key=lambda m: (m // 2 == 0, (m // 2) % 2 != 1 or m // 2 > 1, -m))


def dispatch_kernel(owners, helpers, order, send, gath, zs, zr, xs, xr, cs, cr, own_sem):
    e, h = lax.axis_index("expert"), lax.axis_index("helper")
    hx, hc = flip(h, helpers // 2), flip(h, 1)
    hxc = flip(hc, helpers // 2)
    barrier = pltpu.get_barrier_semaphore()
    for k in order:
        pl.semaphore_signal(barrier, inc=1, device_id=(flip(e, k), h), device_id_type=MESH)
    for other in (hx, hc):
        pl.semaphore_signal(barrier, inc=1, device_id=(e, other), device_id_type=MESH)
    pl.semaphore_wait(barrier, owners + 1)

    def to_owner(k):
        return pltpu.make_async_remote_copy(
            send.at[flip(e, k)], gath.at[h, e], zs.at[k], zr.at[k],
            device_id=(flip(e, k), h), device_id_type=MESH,
        )

    def from_owner(k):
        return pltpu.make_async_remote_copy(
            send.at[flip(e, k)], gath.at[h, flip(e, k)], zs.at[k], zr.at[k],
            device_id=(flip(e, k), h), device_id_type=MESH,
        )

    def across(k):
        block = send.at[e] if k == 0 else gath.at[h, flip(e, k)]
        return pltpu.make_async_remote_copy(
            block, gath.at[h, flip(e, k)], xs.at[k], xr.at[k],
            device_id=(e, hx), device_id_type=MESH,
        )

    def from_across(k):
        return pltpu.make_async_remote_copy(
            send.at[e], gath.at[hx, flip(e, k)], xs.at[k], xr.at[k],
            device_id=(e, hx), device_id_type=MESH,
        )

    def beside(k, far):
        column = hx if far else h
        block = send.at[e] if (k == 0 and not far) else gath.at[column, flip(e, k)]
        return pltpu.make_async_remote_copy(
            block, gath.at[column, flip(e, k)], cs.at[far, k], cr.at[far, k],
            device_id=(e, hc), device_id_type=MESH,
        )

    def from_beside(k, far):
        column = hxc if far else hc
        return pltpu.make_async_remote_copy(
            send.at[e], gath.at[column, flip(e, k)], cs.at[far, k], cr.at[far, k],
            device_id=(e, hc), device_id_type=MESH,
        )

    for k in order:
        to_owner(k).start()
    own = pltpu.make_async_copy(send.at[e], gath.at[h, e], own_sem)
    own.start()
    across(0).start()
    beside(0, 0).start()
    own.wait()
    before = 0
    for k in order:
        from_owner(k).wait_recv()
        across(k).start()
        beside(k, 0).start()
        from_across(before).wait_recv()
        beside(before, 1).start()
        before = k
    from_across(before).wait_recv()
    beside(before, 1).start()
    for k in [0] + order:
        if k:
            to_owner(k).wait_send()
        across(k).wait_send()
        for far in (0, 1):
            beside(k, far).wait_send()
            from_beside(k, far).wait_recv()


def combine_kernel(owners, helpers, order, part, back, own, near, far_in, pair, total, os, ns, nr, xs, xr, zs, zr, last):
    e, h = lax.axis_index("expert"), lax.axis_index("helper")
    hx, hc = flip(h, helpers // 2), flip(h, 1)
    hxc = flip(hc, helpers // 2)
    tiles = part.shape[2]
    barrier = pltpu.get_barrier_semaphore()
    for k in order:
        pl.semaphore_signal(barrier, inc=1, device_id=(flip(e, k), h), device_id_type=MESH)
    for other in (hx, hc):
        pl.semaphore_signal(barrier, inc=1, device_id=(e, other), device_id_type=MESH)
    pl.semaphore_wait(barrier, owners + 1)
    turns = order + [0]

    def load(k, far):
        return pltpu.make_async_copy(part.at[hx if far else h, flip(e, k)], own.at[far, k], os.at[far, k])

    def beside(k, far):
        return pltpu.make_async_remote_copy(
            part.at[hxc if far else hc, flip(e, k)], near.at[far, k], ns.at[far, k], nr.at[far, k],
            device_id=(e, hc), device_id_type=MESH,
        )

    def across(k):
        return pltpu.make_async_remote_copy(
            pair.at[k], far_in.at[k], xs.at[k], xr.at[k], device_id=(e, hx), device_id_type=MESH
        )

    def home(k):
        return pltpu.make_async_remote_copy(
            total.at[k], back.at[e], zs.at[k], zr.at[k],
            device_id=(flip(e, k), h), device_id_type=MESH,
        )

    def from_home(k):
        return pltpu.make_async_remote_copy(
            total.at[k], back.at[flip(e, k)], zs.at[k], zr.at[k],
            device_id=(flip(e, k), h), device_id_type=MESH,
        )

    for far in (1, 0):
        for k in turns:
            beside(k, far).start()
            load(k, far).start()

    waiting = None
    for k in turns:
        load(k, 1).wait()
        beside(k, 1).wait_recv()

        def add_pair(t, carry, k=k):
            pair[k, t] = (own[1, k, t].astype(jnp.float32) + near[1, k, t].astype(jnp.float32)).astype(jnp.bfloat16)
            return carry

        lax.fori_loop(0, tiles, add_pair, 0)
        if waiting is not None:
            across(waiting).start()
        waiting = k
    load(turns[0], 0).wait()
    across(waiting).start()

    waiting = None
    for k in turns:
        if k != turns[0]:
            load(k, 0).wait()
        beside(k, 0).wait_recv()
        across(k).wait_recv()

        def add_all(t, carry, k=k):
            total[k, t] = (
                own[0, k, t].astype(jnp.float32)
                + near[0, k, t].astype(jnp.float32)
                + far_in[k, t].astype(jnp.float32)
            ).astype(jnp.bfloat16)
            return carry

        lax.fori_loop(0, tiles, add_all, 0)
        if waiting is not None:
            home(waiting).start()
        waiting = k
    for k in turns:
        across(k).wait_send()
        for far in (0, 1):
            beside(k, far).wait_send()
    mine = pltpu.make_async_copy(total.at[0], back.at[e], last)
    mine.start()
    for k in order:
        home(k).wait_send()
        from_home(k).wait_recv()
    mine.wait()


def experts_kernel(held, blocks, tiles, counts, x_hbm, wi_hbm, wo_hbm, o_hbm, x, wi, wo, o, todo, x_sem, w_sem, o_sem):
    slabs = x_sem.shape[0]
    slab = blocks * tiles // slabs
    room = blocks * tiles + CHUNK
    width = x.shape[2]

    def x_copy(i):
        return pltpu.make_async_copy(x_hbm.at[pl.ds(i * slab, slab)], x.at[pl.ds(i * slab, slab)], x_sem.at[i])

    def o_copy(i):
        return pltpu.make_async_copy(o.at[pl.ds(i * slab, slab)], o_hbm.at[pl.ds(i * slab, slab)], o_sem.at[i])

    def w_copies(j):
        return (
            pltpu.make_async_copy(wi_hbm.at[j], wi.at[j], w_sem.at[0, j]),
            pltpu.make_async_copy(wo_hbm.at[j], wo.at[j], w_sem.at[1, j]),
        )

    for copy in w_copies(0):
        copy.start()
    for i in range(slabs):
        x_copy(i).start()
    for j in range(1, held):
        for copy in w_copies(j):
            copy.start()

    def clear(i, carry):
        o[i] = jnp.zeros((TILE, width), o.dtype)
        return carry

    lax.fori_loop(0, blocks * tiles, clear, 0)

    chunks = []
    for j in range(held):

        def of_block(b, found, j=j):
            begin = jnp.int32(0)
            for i in range(j):
                begin = begin + counts[b * held + i]
            end = begin + counts[b * held + j]
            first = begin // TILE
            last = jnp.where(end > begin, (end + TILE - 1) // TILE, first)

            def of_tile(t, found):
                low = jnp.maximum(begin - t * TILE, 0)
                high = jnp.minimum(end - t * TILE, TILE)
                todo[j * room + found] = b * tiles + t + low * 65536 + high * 16777216
                return found + 1

            return lax.fori_loop(first, last, of_tile, found)

        found = lax.fori_loop(0, blocks, of_block, jnp.int32(0))
        for i in range(CHUNK):
            todo[j * room + found + i] = 0
        chunks.append((found + CHUNK - 1) // CHUNK)

    for i in range(slabs):
        x_copy(i).wait()
    rows = lax.broadcasted_iota(jnp.int32, (TILE, width), 0)
    for j in range(held):
        for copy in w_copies(j):
            copy.wait()

        def of_chunk(c, carry, j=j):
            entries = [todo[j * room + c * CHUNK + i] for i in range(CHUNK)]
            places = [entry % 65536 for entry in entries]
            taken = jnp.concatenate([x[place] for place in places], axis=0)
            hidden = jnp.maximum(jnp.dot(taken, wi[j], preferred_element_type=jnp.float32), 0.0).astype(jnp.bfloat16)
            made = jnp.dot(hidden, wo[j], preferred_element_type=jnp.float32)
            for i in range(CHUNK):
                low = (entries[i] // 65536) % 256
                high = entries[i] // 16777216
                mine = (rows >= low) & (rows < high)
                old = o[places[i]].astype(jnp.float32)
                o[places[i]] = jnp.where(mine, made[i * TILE : (i + 1) * TILE], old).astype(o.dtype)
            return carry

        lax.fori_loop(0, chunks[j], of_chunk, 0)
    for i in range(slabs):
        o_copy(i).start()
    for i in range(slabs):
        o_copy(i).wait()


def earlier_counts(onehot):
    rows = onehot.shape[0]
    earlier = lax.broadcasted_iota(jnp.int32, (rows, rows), 0) > lax.broadcasted_iota(jnp.int32, (rows, rows), 1)
    return jnp.dot(earlier.astype(jnp.bfloat16), onehot.astype(jnp.bfloat16), preferred_element_type=jnp.float32)


def chosen(onehot, values):
    return jnp.sum(jnp.where(onehot, values, 0.0), axis=1).astype(jnp.int32)


def assign(first, backup, capacity, owners, held):
    columns = jnp.arange(owners * held, dtype=jnp.int32)
    room = capacity.astype(jnp.float32)[None, :]
    onehot = first[:, None] == columns[None, :]
    before = earlier_counts(onehot)
    kept = chosen(onehot, room - before) > 0
    spill = (backup[:, None] == columns[None, :]) & ~kept[:, None]
    spilled = earlier_counts(spill)
    kept_count = jnp.minimum(jnp.sum(onehot.astype(jnp.float32), axis=0, keepdims=True), room)
    counts = kept_count + jnp.sum(spill.astype(jnp.float32), axis=0, keepdims=True)
    same = columns[:, None] // held == columns[None, :] // held
    lower = same & (columns[:, None] < columns[None, :])
    starts = jnp.sum(jnp.where(lower, counts.reshape(-1, 1), 0.0), axis=0, keepdims=True)
    place = jnp.where(kept, chosen(onehot, starts + before), chosen(spill, starts + kept_count + spilled))
    final = jnp.where(kept, first, backup)
    return final // held, place, counts[0].astype(jnp.int32), starts[0].astype(jnp.int32)


def on_device(tokens, gate, expert_ids, backup_ids, capacity, w_in, w_out):
    held = w_in.shape[0]
    owners, helpers = lax.axis_size("expert"), lax.axis_size("helper")
    rows, width = tokens.shape
    experts = held * owners
    most = min(rows, held * 2 * max(6, 3 * rows // (2 * experts)))
    tiles = -(-(13 * rows // (8 * owners)) // TILE)
    block = tiles * TILE
    usable = block - 1
    blocks = owners * helpers
    order = visits(owners)
    f32, bf16 = jnp.float32, jnp.bfloat16
    dma = pltpu.SemaphoreType.DMA
    anywhere = pl.BlockSpec(memory_space=pl.ANY)
    shape = (helpers, owners, tiles, TILE, width)

    group, place, counts, starts = assign(expert_ids[:, 0], backup_ids[:, 0], capacity, owners, held)

    dispatch = pl.pallas_call(
        functools.partial(dispatch_kernel, owners, helpers, order),
        out_shape=jax.ShapeDtypeStruct(shape, bf16),
        in_specs=[pl.BlockSpec(memory_space=pltpu.VMEM)],
        out_specs=anywhere,
        scratch_shapes=[dma((owners,)), dma((owners,)), dma((owners,)), dma((owners,)), dma((2, owners)), dma((2, owners)), dma],
        compiler_params=pltpu.CompilerParams(collective_id=0, has_side_effects=True, vmem_limit_bytes=VMEM_BYTES),
        name="dispatch",
    )
    slabs = 8
    apply = pl.pallas_call(
        functools.partial(experts_kernel, held, blocks, tiles),
        out_shape=jax.ShapeDtypeStruct((blocks * tiles, TILE, width), bf16),
        in_specs=[pl.BlockSpec(memory_space=pltpu.SMEM), anywhere, anywhere, anywhere],
        out_specs=anywhere,
        scratch_shapes=[
            pltpu.VMEM((blocks * tiles, TILE, width), bf16),
            pltpu.VMEM(w_in.shape, bf16),
            pltpu.VMEM(w_out.shape, bf16),
            pltpu.VMEM((blocks * tiles, TILE, width), bf16),
            pltpu.SMEM((held * (blocks * tiles + CHUNK),), jnp.int32),
            dma((slabs,)), dma((2, held)), dma((slabs,)),
        ],
        compiler_params=pltpu.CompilerParams(vmem_limit_bytes=VMEM_BYTES),
        name="experts",
    )
    piece = (tiles, TILE, width)
    combine = pl.pallas_call(
        functools.partial(combine_kernel, owners, helpers, order),
        out_shape=jax.ShapeDtypeStruct((owners,) + piece, bf16),
        in_specs=[anywhere],
        out_specs=anywhere,
        scratch_shapes=[
            pltpu.VMEM((2, owners) + piece, bf16),
            pltpu.VMEM((2, owners) + piece, bf16),
            pltpu.VMEM((owners,) + piece, bf16),
            pltpu.VMEM((owners,) + piece, bf16),
            pltpu.VMEM((owners,) + piece, bf16),
            dma((2, owners)), dma((2, owners)), dma((2, owners)),
            dma((owners,)), dma((owners,)), dma((owners,)), dma((owners,)), dma,
        ],
        compiler_params=pltpu.CompilerParams(collective_id=1, has_side_effects=True, vmem_limit_bytes=VMEM_BYTES),
        name="combine",
    )

    def exchange(number):
        local = place - number * usable
        target = jnp.where((local >= 0) & (local < usable), group * block + local, -1)
        hot = lax.broadcasted_iota(jnp.int32, (owners * block, rows), 0) == target[None, :]
        packed = jnp.dot(hot.astype(bf16), tokens, preferred_element_type=f32).reshape(owners, block, width)
        begin = jnp.clip(starts - number * usable, 0, usable)
        end = jnp.clip(starts + counts - number * usable, 0, usable)
        left = jnp.any(starts + counts > (number + 1) * usable)
        notes = jnp.concatenate(
            [(end - begin).reshape(owners, held), jnp.broadcast_to(left, (owners, 1)).astype(jnp.int32)], axis=1
        )
        notes = jnp.pad(notes, ((0, 0), (0, width - held - 1))).astype(f32)
        is_note = lax.broadcasted_iota(jnp.int32, (owners, block, width), 1) == usable
        packed = jnp.where(is_note, notes[:, None, :], packed).astype(bf16)
        gathered = dispatch(packed.reshape((owners,) + piece))
        said = gathered[:, :, tiles - 1, TILE - 1, : held + 1].astype(jnp.int32)
        made = apply(
            said[:, :, :held].reshape(-1), gathered.reshape(blocks * tiles, TILE, width), w_in, w_out
        )
        back = combine(made.reshape(shape)).reshape(owners * block, width)
        source = target[:, None] == lax.broadcasted_iota(jnp.int32, (rows, owners * block), 1)
        picked = jnp.dot(source.astype(bf16), back, preferred_element_type=f32)
        return (gate[:, None] * picked).astype(bf16), jnp.any(said[:, :, held] > 0), target >= 0

    mixed, more, _ = exchange(0)
    for number in range(1, -(-most // usable)):

        def again(mixed, number=number):
            late, more, here = exchange(number)
            return jnp.where(here[:, None], late, mixed), more

        mixed, more = lax.cond(more, again, lambda mixed: (mixed, jnp.bool_(False)), mixed)
    return mixed


def solution(mesh):
    placed = (
        P(("expert", "helper"), None),
        P(("expert", "helper")),
        P(("expert", "helper"), None),
        P(("expert", "helper"), None),
        P(),
        P("expert", None, "helper"),
        P("expert", "helper", None),
    )
    return jax.shard_map(
        on_device, mesh=mesh, in_specs=placed, out_specs=P(("expert", "helper"), None), check_vma=False
    )
```

```python
import functools

import jax
import jax.numpy as jnp
from jax import lax
from jax.experimental import pallas as pl
from jax.experimental.pallas import tpu as pltpu
from jax.sharding import PartitionSpec as P

MESH = pl.DeviceIdType.MESH
TILE = 16
VMEM_BYTES = 63 * 2**20


def exclusive(index, mask, limit):
    out, bit = 0, 1
    while bit < limit:
        one, two = (index // bit) % 2, (mask // bit) % 2
        out = out + bit * (one + two - 2 * one * two)
        bit *= 2
    return out


def outward(owners):
    steps = [step ^ (step // 2) for step in range(2, owners)]
    return steps + [1]


def homeward(owners):
    ends = sorted(range(owners), key=lambda m: (m // 8, (6, 4, 1, 0)[m // 2 % 4], (m if m // 2 == 3 else -m)))
    middle = sorted(range(owners), key=lambda m: (m // 8, (3, 0, 1, 6)[m // 2 % 4], (m if m // 2 % 4 in (1, 3) else -m)))
    return ends, middle


def windows(held, tiles):
    reach = [min(tiles, -(-(4 * i + 5) * tiles // 13)) for i in range(held // 2)]
    front = [(0, r) for r in reach]
    rear = [(tiles - r, tiles) for r in reach]
    return front + rear[::-1]


def layer_kernel(
    owners, helpers, held, send, wi_hbm, wo_hbm, back, flags, x, o, near, far_in, wi, wo,
    zs, zr, xs, xr, cs, cr, gs, gr, fs, fr, hs, hr, ws, last,
):
    e, h = lax.axis_index("expert"), lax.axis_index("helper")
    hx, hc = exclusive(h, helpers // 2, helpers), exclusive(h, 1, helpers)
    hxc = exclusive(hc, helpers // 2, helpers)
    tiles, width = x.shape[2], x.shape[4]
    f32, bf16 = jnp.float32, jnp.bfloat16

    def partner(k):
        return exclusive(e, k, owners)

    def to_owner(k):
        return pltpu.make_async_remote_copy(
            send.at[partner(k)], x.at[h, e], zs.at[k], zr.at[k], device_id=(partner(k), h), device_id_type=MESH
        )

    def from_owner(k):
        return pltpu.make_async_remote_copy(
            send.at[e], x.at[h, partner(k)], zs.at[k], zr.at[k], device_id=(partner(k), h), device_id_type=MESH
        )

    def across(k):
        return pltpu.make_async_remote_copy(
            x.at[h, partner(k)], x.at[h, partner(k)], xs.at[k], xr.at[k], device_id=(e, hx), device_id_type=MESH
        )

    def from_across(k):
        return pltpu.make_async_remote_copy(
            send.at[e], x.at[hx, partner(k)], xs.at[k], xr.at[k], device_id=(e, hx), device_id_type=MESH
        )

    def beside(k, far):
        block = x.at[hx if far else h, partner(k)]
        return pltpu.make_async_remote_copy(
            block, block, cs.at[far, k], cr.at[far, k], device_id=(e, hc), device_id_type=MESH
        )

    def from_beside(k, far):
        return pltpu.make_async_remote_copy(
            send.at[e], x.at[hxc if far else hc, partner(k)], cs.at[far, k], cr.at[far, k],
            device_id=(e, hc), device_id_type=MESH,
        )

    def give(k, far):
        return pltpu.make_async_remote_copy(
            o.at[hxc if far else hc, partner(k)], near.at[far, k], gs.at[far, k], gr.at[far, k],
            device_id=(e, hc), device_id_type=MESH,
        )

    def pair_over(k):
        return pltpu.make_async_remote_copy(
            o.at[hx, partner(k)], far_in.at[k], fs.at[k], fr.at[k], device_id=(e, hx), device_id_type=MESH
        )

    def home(k):
        return pltpu.make_async_remote_copy(
            o.at[h, partner(k)], back.at[e], hs.at[k], hr.at[k], device_id=(partner(k), h), device_id_type=MESH
        )

    def from_home(k):
        return pltpu.make_async_remote_copy(
            o.at[h, e], back.at[partner(k)], hs.at[k], hr.at[k], device_id=(partner(k), h), device_id_type=MESH
        )

    def weights(j):
        return (
            pltpu.make_async_copy(wi_hbm.at[j], wi.at[j], ws.at[0, j]),
            pltpu.make_async_copy(wo_hbm.at[j], wo.at[j], ws.at[1, j]),
        )

    for j in range(held):
        for copy in weights(j):
            copy.start()
    barrier = pltpu.get_barrier_semaphore()
    for k in range(1, owners):
        pl.semaphore_signal(barrier, inc=1, device_id=(partner(k), h), device_id_type=MESH)
    for other in (hx, hc):
        pl.semaphore_signal(barrier, inc=1, device_id=(e, other), device_id_type=MESH)

    def fill(t, carry):
        x[h, e, t] = send[e, t]
        return carry

    lax.fori_loop(0, tiles, fill, 0)
    pl.semaphore_wait(barrier, owners + 1)
    for k in outward(owners):
        to_owner(k).start()
    across(0).start()
    beside(0, 0).start()

    def clear(i, carry):
        o[i // (owners * tiles), (i // tiles) % owners, i % tiles] = jnp.zeros((TILE, width), bf16)
        return carry

    lax.fori_loop(0, helpers * owners * tiles, clear, 0)
    flags[...] = jnp.zeros(flags.shape, f32)
    for j in range(held):
        for copy in weights(j):
            copy.wait()

    in_middle = exclusive((e // 2) % 2, (e // 4) % 2, 2)
    plan = [(min(one, two), one + in_middle * (two - one)) for one, two in zip(*homeward(owners))]

    def add_pair(k):
        give(k, 1).wait_recv()

        def one_tile(t, carry):
            o[hx, partner(k), t] = (o[hx, partner(k), t].astype(f32) + near[1, k, t].astype(f32)).astype(bf16)
            return carry

        lax.fori_loop(0, tiles, one_tile, 0)

    def add_all(k):
        give(k, 0).wait_recv()
        pair_over(k).wait_recv()

        def one_tile(t, carry):
            o[h, partner(k), t] = (
                o[h, partner(k), t].astype(f32) + near[0, k, t].astype(f32) + far_in[k, t].astype(f32)
            ).astype(bf16)
            return carry

        lax.fori_loop(0, tiles, one_tile, 0)

    def compute(k):
        source = partner(k)
        notes = [x[c, source, tiles - 1][TILE - 1 : TILE, :128].astype(f32) for c in range(helpers)]
        seen = flags[0:1, :]
        for note in notes:
            seen = jnp.maximum(seen, note)
        flags[0:1, :] = seen
        for j, (low, high) in enumerate(windows(held, tiles)):
            size = (high - low) * TILE
            taken = jnp.concatenate([x[c, source, low:high].reshape(size, width) for c in range(helpers)], axis=0)
            hidden = jnp.maximum(jnp.dot(taken, wi[j], preferred_element_type=f32), 0.0).astype(bf16)
            made = jnp.dot(hidden, wo[j], preferred_element_type=f32)
            row = (lax.broadcasted_iota(jnp.int32, (size, width), 0) + low * TILE).astype(f32)
            for c in range(helpers):
                mine = (row >= notes[c][:, j : j + 1]) & (row < notes[c][:, held + j : held + j + 1])
                old = o[c, source, low:high].reshape(size, width).astype(f32)
                new = jnp.where(mine, made[c * size : (c + 1) * size], old).astype(bf16)
                o[c, source, low:high] = new.reshape(high - low, TILE, width)

    early = 2

    def step(i, carry):
        k = exclusive(i, i // 2, owners)

        @pl.when(i + 1 < owners)
        def _():
            ahead = exclusive(i + 1, (i + 1) // 2, owners)
            from_owner(ahead).wait_recv()
            across(ahead).start()
            beside(ahead, 0).start()

        from_across(k).wait_recv()
        beside(k, 1).start()

        @pl.when(i > 0)
        def _():
            before = exclusive(i - 1, (i - 1) // 2, owners)
            give(before, 1).start()
            give(before, 0).start()

        @pl.when(i + 1 == owners)
        def _():
            for _, first in plan[:early]:
                add_pair(first)
            for _, first in plan[:early]:
                pair_over(first).start()

        from_beside(k, 0).wait_recv()
        from_beside(k, 1).wait_recv()
        compute(k)
        return carry

    lax.fori_loop(0, owners, step, 0)
    final = (owners - 1) ^ ((owners - 1) // 2)
    waiting = None
    for n, (_, k) in enumerate(plan[early:]):
        if n == 1:
            give(final, 1).start()
            give(final, 0).start()
        add_pair(k)
        if waiting is not None:
            pair_over(waiting).start()
        waiting = k
    add_all(plan[0][1])
    pair_over(waiting).start()

    def send_home(always, k):
        if always:
            home(k).start()
        else:

            @pl.when(k > 0)
            def _():
                home(k).start()

    waiting = plan[0]
    for always, k in plan[1:]:
        add_all(k)
        send_home(*waiting)
        waiting = always, k
    for k in range(owners):
        across(k).wait_send()
        pair_over(k).wait_send()
        for far in (0, 1):
            beside(k, far).wait_send()
            give(k, far).wait_send()
        if k:
            to_owner(k).wait_send()
    send_home(*waiting)
    mine = pltpu.make_async_copy(o.at[h, e], back.at[e], last)
    mine.start()
    for k in range(1, owners):
        home(k).wait_send()
        from_home(k).wait_recv()
    mine.wait()


def earlier_counts(onehot):
    rows = onehot.shape[0]
    earlier = lax.broadcasted_iota(jnp.int32, (rows, rows), 0) > lax.broadcasted_iota(jnp.int32, (rows, rows), 1)
    return jnp.dot(earlier.astype(jnp.bfloat16), onehot.astype(jnp.bfloat16), preferred_element_type=jnp.float32)


def chosen(onehot, values):
    return jnp.sum(jnp.where(onehot, values, 0.0), axis=1).astype(jnp.int32)


def assign(first, backup, capacity, experts):
    columns = jnp.arange(experts, dtype=jnp.int32)
    room = capacity.astype(jnp.float32)[None, :]
    onehot = first[:, None] == columns[None, :]
    before = earlier_counts(onehot)
    kept = chosen(onehot, room - before) > 0
    spill = (backup[:, None] == columns[None, :]) & ~kept[:, None]
    spilled = earlier_counts(spill)
    kept_count = jnp.minimum(jnp.sum(onehot.astype(jnp.float32), axis=0, keepdims=True), room)
    counts = kept_count + jnp.sum(spill.astype(jnp.float32), axis=0, keepdims=True)
    final = (onehot & kept[:, None]) | spill
    rank = jnp.where(kept[:, None], before, kept_count + spilled)
    return final, rank, counts[0].astype(jnp.int32)


def on_device(tokens, gate, expert_ids, backup_ids, capacity, w_in, w_out):
    held = w_in.shape[0]
    owners, helpers = lax.axis_size("expert"), lax.axis_size("helper")
    rows, width = tokens.shape
    experts = held * owners
    tiles = -(-(13 * rows // (8 * owners)) // TILE)
    block = tiles * TILE
    usable = block - 1
    f32, bf16 = jnp.float32, jnp.bfloat16
    dma = pltpu.SemaphoreType.DMA
    anywhere = pl.BlockSpec(memory_space=pl.ANY)
    vmem = pl.BlockSpec(memory_space=pltpu.VMEM)
    piece = (tiles, TILE, width)

    layer = pl.pallas_call(
        functools.partial(layer_kernel, owners, helpers, held),
        out_shape=(jax.ShapeDtypeStruct((owners,) + piece, bf16), jax.ShapeDtypeStruct((8, 128), f32)),
        in_specs=[vmem, anywhere, anywhere],
        out_specs=(anywhere, vmem),
        scratch_shapes=[
            pltpu.VMEM((helpers, owners) + piece, bf16),
            pltpu.VMEM((helpers, owners) + piece, bf16),
            pltpu.VMEM((2, owners) + piece, bf16),
            pltpu.VMEM((owners,) + piece, bf16),
            pltpu.VMEM(w_in.shape, bf16),
            pltpu.VMEM(w_out.shape, bf16),
            dma((owners,)), dma((owners,)), dma((owners,)), dma((owners,)),
            dma((2, owners)), dma((2, owners)), dma((2, owners)), dma((2, owners)),
            dma((owners,)), dma((owners,)), dma((owners,)), dma((owners,)),
            dma((2, held)), dma,
        ],
        compiler_params=pltpu.CompilerParams(collective_id=0, has_side_effects=True, vmem_limit_bytes=VMEM_BYTES),
        name="layer",
    )

    final, rank, counts = assign(expert_ids[:, 0], backup_ids[:, 0], capacity, experts)
    spans = windows(held, tiles)

    def exchange(done):
        todo = (counts - done).reshape(owners, held)
        takes, starts, used = [None] * held, [None] * held, 0
        for j in range(held // 2):
            takes[j] = jnp.minimum(todo[:, j], spans[j][1] * TILE - used)
            if spans[j][1] == tiles:
                takes[j] = jnp.minimum(takes[j], usable - used)
            starts[j] = used + jnp.zeros_like(takes[j])
            used = used + takes[j]
        end = usable
        for j in range(held - 1, held // 2 - 1, -1):
            takes[j] = jnp.minimum(jnp.minimum(todo[:, j], end - spans[j][0] * TILE), end - used)
            starts[j] = end - takes[j]
            end = end - takes[j]
        takes, starts = jnp.stack(takes, axis=1), jnp.stack(starts, axis=1)
        left = jnp.any(todo > takes)
        offset = rank - done.astype(f32)[None, :]
        flat = takes.reshape(1, experts).astype(f32)
        here = final & (offset >= 0) & (offset < flat)
        base = (starts + jnp.arange(owners, dtype=jnp.int32)[:, None] * block).reshape(1, experts).astype(f32)
        target = jnp.sum(jnp.where(here, offset + base + 1, 0.0), axis=1).astype(jnp.int32) - 1
        hot = lax.broadcasted_iota(jnp.int32, (owners * block, rows), 0) == target[None, :]
        packed = jnp.dot(hot.astype(bf16), tokens, preferred_element_type=f32).reshape(owners, block, width)
        flag = jnp.broadcast_to(left, (owners, 1)).astype(jnp.int32)
        notes = jnp.concatenate([starts, starts + takes, flag], axis=1)
        notes = jnp.pad(notes, ((0, 0), (0, width - 2 * held - 1))).astype(f32)
        is_note = lax.broadcasted_iota(jnp.int32, (owners, block, width), 1) == usable
        packed = jnp.where(is_note, notes[:, None, :], packed).astype(bf16)
        back, flags = layer(packed.reshape((owners,) + piece), w_in, w_out)
        source = target[:, None] == lax.broadcasted_iota(jnp.int32, (rows, owners * block), 1)
        picked = jnp.dot(source.astype(bf16), back.reshape(owners * block, width), preferred_element_type=f32)
        return (gate[:, None] * picked).astype(bf16), target >= 0, done + takes.reshape(experts), flags[0, 2 * held] > 0

    mixed, _, done, more = exchange(jnp.zeros_like(counts))

    def again(state):
        mixed, done, _ = state
        late, here, done, more = exchange(done)
        return jnp.where(here[:, None], late, mixed), done, more

    return lax.while_loop(lambda state: state[2], again, (mixed, done, more))[0]


def solution(mesh):
    placed = (
        P(("expert", "helper"), None),
        P(("expert", "helper")),
        P(("expert", "helper"), None),
        P(("expert", "helper"), None),
        P(),
        P("expert", None, "helper"),
        P("expert", "helper", None),
    )
    return jax.shard_map(
        on_device, mesh=mesh, in_specs=placed, out_specs=P(("expert", "helper"), None), check_vma=False
    )
```

```python
import functools

import jax
import jax.numpy as jnp
from jax import lax
from jax.experimental import pallas as pl
from jax.experimental.pallas import tpu as pltpu
from jax.sharding import PartitionSpec as P

MESH = pl.DeviceIdType.MESH
TILE = 16
VMEM_BYTES = 63 * 2**20
AHEAD = 2
SEND = (1, 3, 2, 6, 7, 5, 4)
TAKE = (0, 1, 3, 2, 6, 7, 5, 4)
RETURN_ENDS = (6, 7, 5, 4, 3, 2, 1, 0)
RETURN_MIDDLE = (6, 7, 2, 3, 5, 4, 1, 0)


def exclusive(index, mask, limit):
    out, bit = 0, 1
    while bit < limit:
        one, two = (index // bit) % 2, (mask // bit) % 2
        out = out + bit * (one + two - 2 * one * two)
        bit *= 2
    return out


def masks(order, owners):
    return [high + low for high in range(0, owners, 8) for low in order if high + low < owners]


def windows(held, tiles):
    reach = [min(tiles, -(-(4 * i + 5) * tiles // 13)) for i in range(held // 2)]
    front = [(0, r) for r in reach]
    rear = [(tiles - r, tiles) for r in reach]
    return front + rear[::-1]


def layer_kernel(
    owners, helpers, held, send, wi_hbm, wo_hbm, back, flags, x, o, near, far_in, wi, wo,
    zs, zr, xs, xr, cs, cr, gs, gr, fs, fr, hs, hr, ws, last,
):
    e, h = lax.axis_index("expert"), lax.axis_index("helper")
    hx, hc = exclusive(h, helpers // 2, helpers), exclusive(h, 1, helpers)
    hxc = exclusive(hc, helpers // 2, helpers)
    tiles, width = x.shape[2], x.shape[4]
    f32, bf16 = jnp.float32, jnp.bfloat16

    in_middle = exclusive((e // 2) % 2, (e // 4) % 2, 2)

    def partner(k):
        return exclusive(e, k, owners)

    def to_owner(k):
        return pltpu.make_async_remote_copy(
            send.at[partner(k)], x.at[h, e], zs.at[k], zr.at[k], device_id=(partner(k), h), device_id_type=MESH
        )

    def from_owner(k):
        return pltpu.make_async_remote_copy(
            send.at[e], x.at[h, partner(k)], zs.at[k], zr.at[k], device_id=(partner(k), h), device_id_type=MESH
        )

    def across(k):
        return pltpu.make_async_remote_copy(
            x.at[h, partner(k)], x.at[h, partner(k)], xs.at[k], xr.at[k], device_id=(e, hx), device_id_type=MESH
        )

    def from_across(k):
        return pltpu.make_async_remote_copy(
            send.at[e], x.at[hx, partner(k)], xs.at[k], xr.at[k], device_id=(e, hx), device_id_type=MESH
        )

    def beside(k, far):
        block = x.at[hx if far else h, partner(k)]
        return pltpu.make_async_remote_copy(
            block, block, cs.at[far, k], cr.at[far, k], device_id=(e, hc), device_id_type=MESH
        )

    def from_beside(k, far):
        return pltpu.make_async_remote_copy(
            send.at[e], x.at[hxc if far else hc, partner(k)], cs.at[far, k], cr.at[far, k],
            device_id=(e, hc), device_id_type=MESH,
        )

    def give(k, far):
        return pltpu.make_async_remote_copy(
            o.at[hxc if far else hc, partner(k)], near.at[far, k], gs.at[far, k], gr.at[far, k],
            device_id=(e, hc), device_id_type=MESH,
        )

    def pair_over(k):
        return pltpu.make_async_remote_copy(
            o.at[hx, partner(k)], far_in.at[k], fs.at[k], fr.at[k], device_id=(e, hx), device_id_type=MESH
        )

    def home(k):
        return pltpu.make_async_remote_copy(
            o.at[h, partner(k)], back.at[e], hs.at[k], hr.at[k], device_id=(partner(k), h), device_id_type=MESH
        )

    def from_home(k):
        return pltpu.make_async_remote_copy(
            o.at[h, e], back.at[partner(k)], hs.at[k], hr.at[k], device_id=(partner(k), h), device_id_type=MESH
        )

    def weights(j):
        return (
            pltpu.make_async_copy(wi_hbm.at[j], wi.at[j], ws.at[0, j]),
            pltpu.make_async_copy(wo_hbm.at[j], wo.at[j], ws.at[1, j]),
        )

    for j in range(held):
        for copy in weights(j):
            copy.start()
    barrier = pltpu.get_barrier_semaphore()
    for k in range(1, owners):
        pl.semaphore_signal(barrier, inc=1, device_id=(partner(k), h), device_id_type=MESH)
    for other in (hx, hc):
        pl.semaphore_signal(barrier, inc=1, device_id=(e, other), device_id_type=MESH)

    def fill(t, carry):
        x[h, e, t] = send[e, t]
        return carry

    lax.fori_loop(0, tiles, fill, 0)
    pl.semaphore_wait(barrier, owners + 1)
    across(0).start()
    beside(0, 0).start()
    for k in masks((0,) + SEND, owners)[1:]:
        to_owner(k).start()

    flags[...] = jnp.zeros(flags.shape, f32)

    plan = [(min(one, two), one + in_middle * (two - one)) for one, two in zip(masks(RETURN_ENDS, owners), masks(RETURN_MIDDLE, owners))]

    def add_pair(k):
        give(k, 1).wait_recv()

        def one_tile(t, carry):
            o[hx, partner(k), t] = (o[hx, partner(k), t].astype(f32) + near[1, k, t].astype(f32)).astype(bf16)
            return carry

        lax.fori_loop(0, tiles, one_tile, 0)

    def add_all(k):
        give(k, 0).wait_recv()
        pair_over(k).wait_recv()

        def one_tile(t, carry):
            o[h, partner(k), t] = (
                o[h, partner(k), t].astype(f32) + near[0, k, t].astype(f32) + far_in[k, t].astype(f32)
            ).astype(bf16)
            return carry

        lax.fori_loop(0, tiles, one_tile, 0)

    def compute(k):
        source = partner(k)
        notes = [x[c, source, tiles - 1][TILE - 1 : TILE, :128].astype(f32) for c in range(helpers)]
        seen = flags[0:1, :]
        for note in notes:
            seen = jnp.maximum(seen, note)
        flags[0:1, :] = seen
        reached = 0
        spans = windows(held, tiles)
        for j in sorted(range(held), key=lambda j: (spans[j][0] - spans[j][1], j)):
            low, high = spans[j]
            size = (high - low) * TILE
            taken = jnp.concatenate([x[c, source, low:high].reshape(size, width) for c in range(helpers)], axis=0)
            hidden = jnp.maximum(jnp.dot(taken, wi[j], preferred_element_type=f32), 0.0).astype(bf16)
            made = jnp.dot(hidden, wo[j], preferred_element_type=f32)
            row = (lax.broadcasted_iota(jnp.int32, (size, width), 0) + low * TILE).astype(f32)
            fresh = max(low, min(reached, high))
            for c in range(helpers):
                mine = (row >= notes[c][:, j : j + 1]) & (row < notes[c][:, held + j : held + j + 1])
                own = made[c * size : (c + 1) * size]
                if fresh > low:
                    upto = (fresh - low) * TILE
                    old = o[c, source, low:fresh].reshape(upto, width).astype(f32)
                    new = jnp.where(mine[:upto], own[:upto], old).astype(bf16)
                    o[c, source, low:fresh] = new.reshape(fresh - low, TILE, width)
                if high > fresh:
                    after = (fresh - low) * TILE
                    new = jnp.where(mine[after:], own[after:], 0.0).astype(bf16)
                    o[c, source, fresh:high] = new.reshape(high - fresh, TILE, width)
            reached = max(reached, high)

    def give_both(k):
        give(k, 1).start()
        give(k, 0).start()

    def start_home(always, k):
        if always:
            home(k).start()
        else:

            @pl.when(k > 0)
            def _():
                home(k).start()

    def send_pairs(turns):
        for n, (_, k) in enumerate(turns):
            add_pair(k)
            if n:
                pair_over(turns[n - 1][1]).start()
        return turns[-1:]

    taken = masks(TAKE, owners)

    def at(i):
        k = 0
        for n, mask in enumerate(taken):
            k = k + mask * jnp.where(i == n, 1, 0)
        return k

    def forward(k):
        from_owner(k).wait_recv()
        across(k).start()
        beside(k, 0).start()

    for k in taken[1:AHEAD]:
        forward(k)
    for j in range(held):
        for copy in weights(j):
            copy.wait()

    def step(i, carry):
        k = at(i)

        @pl.when(i + AHEAD < owners)
        def _():
            forward(at(i + AHEAD))

        from_across(k).wait_recv()
        beside(k, 1).start()

        @pl.when(i > 0)
        def _():
            give_both(at(i - 1))

        for n, turns in ((owners - 2, plan[:1]), (owners - 1, plan[1:3])):

            @pl.when(i == n)
            def _(turns=turns):
                for _, late in send_pairs(turns):
                    pair_over(late).start()

        from_beside(k, 0).wait_recv()
        from_beside(k, 1).wait_recv()
        compute(k)
        return carry

    lax.fori_loop(0, owners, step, 0)
    for k in range(1, owners):
        to_owner(k).wait_send()
    give_both(taken[-1])
    late = send_pairs(plan[3:])
    add_all(plan[0][1])
    pair_over(late[0][1]).start()
    waiting = plan[0]
    for always, k in plan[1:]:
        add_all(k)
        start_home(*waiting)
        waiting = always, k
    for k in range(owners):
        across(k).wait_send()
        pair_over(k).wait_send()
        for far in (0, 1):
            beside(k, far).wait_send()
            give(k, far).wait_send()
    start_home(*waiting)
    mine = pltpu.make_async_copy(o.at[h, e], back.at[e], last)
    mine.start()
    for k in range(1, owners):
        home(k).wait_send()
        from_home(k).wait_recv()
    mine.wait()


def pack_kernel(owners, held, block, spans, first, backup, capacity, done, tokens, send, where, takes_out):
    f32, bf16, i32 = jnp.float32, jnp.bfloat16, jnp.int32
    experts, rows, width, lanes = owners * held, first.shape[1], tokens.shape[1], 128
    usable, tiles = block - 1, block // TILE
    room = capacity[...].astype(f32)
    expert = lax.broadcasted_iota(i32, (experts, rows), 0)
    earlier = (
        lax.broadcasted_iota(i32, (lanes, lanes), 0) < lax.broadcasted_iota(i32, (lanes, lanes), 1)
    ).astype(f32).astype(bf16)

    def ranks(hit):
        pieces = [hit[:, at : at + lanes] for at in range(0, rows, lanes)]
        inner = jnp.dot(jnp.concatenate(pieces, axis=0).astype(bf16), earlier, preferred_element_type=f32)
        total, out = jnp.zeros((experts, 1), f32), []
        for n, piece in enumerate(pieces):
            out.append(inner[n * experts : (n + 1) * experts] + total)
            total = total + jnp.sum(piece, axis=1, keepdims=True)
        return jnp.concatenate(out, axis=1), total

    chosen = jnp.where(expert == first[...], 1.0, 0.0)
    before, named = ranks(chosen)
    kept = jnp.where(before < room, chosen, 0.0)
    stays = jnp.max(kept, axis=0, keepdims=True)
    spill = jnp.where(expert == backup[...], 1.0 - stays, 0.0)
    spilled, extra = ranks(spill)
    kept_count = jnp.minimum(named, room)
    final = kept + spill
    rank = jnp.where(kept > 0.0, before, kept_count + spilled) - done[...]
    todo = jnp.broadcast_to(kept_count + extra - done[...], (experts, lanes))

    turn = lax.broadcasted_iota(i32, (experts, lanes), 0) % held
    same = (
        lax.broadcasted_iota(i32, (experts, experts), 0) // held == lax.broadcasted_iota(i32, (experts, experts), 1) // held
    ).astype(f32).astype(bf16)

    def group_sum(values):
        return jnp.dot(same, values.astype(bf16), preferred_element_type=f32)

    takes, starts = jnp.zeros((experts, lanes), f32), jnp.zeros((experts, lanes), f32)
    used = jnp.zeros((experts, lanes), f32)
    for j in range(held // 2):
        take = jnp.minimum(todo, min(spans[j][1] * TILE, usable) - used)
        takes = jnp.where(turn == j, take, takes)
        starts = jnp.where(turn == j, used, starts)
        used = used + group_sum(jnp.where(turn == j, take, 0.0))
    end = jnp.full((experts, lanes), float(usable), f32)
    for j in range(held - 1, held // 2 - 1, -1):
        take = jnp.minimum(jnp.minimum(todo, end - spans[j][0] * TILE), end - used)
        takes = jnp.where(turn == j, take, takes)
        starts = jnp.where(turn == j, end - take, starts)
        end = end - group_sum(jnp.where(turn == j, take, 0.0))
    takes_out[...] = takes
    left = jnp.max(todo - takes, axis=0, keepdims=True)

    here = jnp.where((rank >= 0.0) & (rank < takes[:, :1]), final, 0.0)
    base = starts[:, :1] + (lax.broadcasted_iota(i32, (experts, 1), 0) // held * block + 1).astype(f32)
    place = jnp.sum(here * (rank + base), axis=0, keepdims=True).astype(i32) - 1
    where[...] = jnp.broadcast_to(place, where.shape)

    lane = lax.broadcasted_iota(i32, (experts, lanes), 1)
    notes = jnp.where(lane == turn, starts, jnp.where(lane == held + turn, starts + takes, 0.0))
    notes = group_sum(notes)
    notes = jnp.where(lane == 2 * held, jnp.where(left > 0.0, 1.0, 0.0), notes)
    last = lax.broadcasted_iota(i32, (block, lanes), 0) == usable
    data = tokens[...]
    for group in range(owners):
        hot = jnp.where(lax.broadcasted_iota(i32, (block, rows), 0) + group * block == place, 1.0, 0.0).astype(bf16)
        packed = jnp.dot(hot, data, preferred_element_type=f32)
        note = jnp.where(last, notes[group * held : group * held + 1, :], packed[:, :lanes])
        packed = jnp.concatenate([note, packed[:, lanes:]], axis=1).astype(bf16)
        send[group] = packed.reshape(tiles, TILE, width)


def pack(owners, held, tiles, first, backup, capacity, done, tokens):
    rows, width = tokens.shape
    experts = owners * held
    return pl.pallas_call(
        functools.partial(pack_kernel, owners, held, tiles * TILE, windows(held, tiles)),
        out_shape=(
            jax.ShapeDtypeStruct((owners, tiles, TILE, width), jnp.bfloat16),
            jax.ShapeDtypeStruct((8, rows), jnp.int32),
            jax.ShapeDtypeStruct((experts, 128), jnp.float32),
        ),
        in_specs=[pl.BlockSpec(memory_space=pltpu.VMEM)] * 5,
        out_specs=[pl.BlockSpec(memory_space=pltpu.VMEM)] * 3,
        compiler_params=pltpu.CompilerParams(vmem_limit_bytes=40 * 2**20),
        name="pack",
    )(first, backup, capacity, done, tokens)


def on_device(tokens, gate, expert_ids, backup_ids, capacity, w_in, w_out):
    held = w_in.shape[0]
    owners, helpers = lax.axis_size("expert"), lax.axis_size("helper")
    rows, width = tokens.shape
    experts = held * owners
    tiles = -(-(13 * rows // (8 * owners)) // TILE)
    block = tiles * TILE
    f32, bf16 = jnp.float32, jnp.bfloat16
    dma = pltpu.SemaphoreType.DMA
    anywhere = pl.BlockSpec(memory_space=pl.ANY)
    vmem = pl.BlockSpec(memory_space=pltpu.VMEM)
    piece = (tiles, TILE, width)

    layer = pl.pallas_call(
        functools.partial(layer_kernel, owners, helpers, held),
        out_shape=(jax.ShapeDtypeStruct((owners,) + piece, bf16), jax.ShapeDtypeStruct((8, 128), f32)),
        in_specs=[vmem, anywhere, anywhere],
        out_specs=(anywhere, vmem),
        scratch_shapes=[
            pltpu.VMEM((helpers, owners) + piece, bf16),
            pltpu.VMEM((helpers, owners) + piece, bf16),
            pltpu.VMEM((2, owners) + piece, bf16),
            pltpu.VMEM((owners,) + piece, bf16),
            pltpu.VMEM(w_in.shape, bf16),
            pltpu.VMEM(w_out.shape, bf16),
            dma((owners,)), dma((owners,)), dma((owners,)), dma((owners,)),
            dma((2, owners)), dma((2, owners)), dma((2, owners)), dma((2, owners)),
            dma((owners,)), dma((owners,)), dma((owners,)), dma((owners,)),
            dma((2, held)), dma,
        ],
        compiler_params=pltpu.CompilerParams(collective_id=0, has_side_effects=True, vmem_limit_bytes=VMEM_BYTES),
        name="layer",
    )

    first, backup = expert_ids.reshape(1, rows), backup_ids.reshape(1, rows)
    room = capacity.reshape(experts, 1)

    def exchange(done):
        send, places, takes = pack(owners, held, tiles, first, backup, room, done, tokens)
        back, flags = layer(send, w_in, w_out)
        target = places[0]
        source = target[:, None] == lax.broadcasted_iota(jnp.int32, (rows, owners * block), 1)
        picked = jnp.dot(source.astype(bf16), back.reshape(owners * block, width), preferred_element_type=f32)
        return (gate[:, None] * picked).astype(bf16), target >= 0, done + takes[:, :1], flags[0, 2 * held] > 0

    mixed, _, done, more = exchange(jnp.zeros((experts, 1), f32))

    def again(state):
        mixed, done, _ = state
        late, here, done, more = exchange(done)
        return jnp.where(here[:, None], late, mixed), done, more

    return lax.while_loop(lambda state: state[2], again, (mixed, done, more))[0]


def solution(mesh):
    placed = (
        P(("expert", "helper"), None),
        P(("expert", "helper")),
        P(("expert", "helper"), None),
        P(("expert", "helper"), None),
        P(),
        P("expert", None, "helper"),
        P("expert", "helper", None),
    )
    return jax.shard_map(
        on_device, mesh=mesh, in_specs=placed, out_specs=P(("expert", "helper"), None), check_vma=False
    )
```

```python
import functools

import jax
import jax.numpy as jnp
from jax import lax
from jax.experimental import pallas as pl
from jax.experimental.pallas import tpu as pltpu
from jax.sharding import PartitionSpec as P

MESH = pl.DeviceIdType.MESH
TILE = 16
VMEM_BYTES = 63 * 2**20
AHEAD = 2
SEND = (1, 3, 2, 6, 7, 5, 4)
TAKE = (0, 1, 3, 2, 6, 7, 5, 4)
RETURN_ENDS = (6, 7, 5, 4, 3, 2, 1, 0)
RETURN_MIDDLE = (6, 7, 2, 3, 5, 4, 1, 0)


def exclusive(index, mask, limit):
    out, bit = 0, 1
    while bit < limit:
        one, two = (index // bit) % 2, (mask // bit) % 2
        out = out + bit * (one + two - 2 * one * two)
        bit *= 2
    return out


def masks(order, owners):
    return [high + low for high in range(0, owners, 8) for low in order if high + low < owners]


def windows(held, tiles):
    reach = [min(tiles, -(-(4 * i + 5) * tiles // 13)) for i in range(held // 2)]
    front = [(0, r) for r in reach]
    rear = [(tiles - r, tiles) for r in reach]
    return front + rear[::-1]


def layer_kernel(
    owners, helpers, held, send, places, wi_hbm, wo_hbm, picked, flags, back, x, o, near, far_in, wi, wo,
    zs, zr, xs, xr, cs, cr, gs, gr, fs, fr, hs, hr, ws,
):
    e, h = lax.axis_index("expert"), lax.axis_index("helper")
    hx, hc = exclusive(h, helpers // 2, helpers), exclusive(h, 1, helpers)
    hxc = exclusive(hc, helpers // 2, helpers)
    tiles, width = x.shape[2], x.shape[4]
    rows, block = places.shape[1], x.shape[2] * TILE
    f32, bf16 = jnp.float32, jnp.bfloat16

    in_middle = exclusive((e // 2) % 2, (e // 4) % 2, 2)

    def partner(k):
        return exclusive(e, k, owners)

    def to_owner(k):
        return pltpu.make_async_remote_copy(
            send.at[partner(k)], x.at[h, e], zs.at[k], zr.at[k], device_id=(partner(k), h), device_id_type=MESH
        )

    def from_owner(k):
        return pltpu.make_async_remote_copy(
            send.at[e], x.at[h, partner(k)], zs.at[k], zr.at[k], device_id=(partner(k), h), device_id_type=MESH
        )

    def across(k):
        return pltpu.make_async_remote_copy(
            x.at[h, partner(k)], x.at[h, partner(k)], xs.at[k], xr.at[k], device_id=(e, hx), device_id_type=MESH
        )

    def from_across(k):
        return pltpu.make_async_remote_copy(
            send.at[e], x.at[hx, partner(k)], xs.at[k], xr.at[k], device_id=(e, hx), device_id_type=MESH
        )

    def beside(k, far):
        block = x.at[hx if far else h, partner(k)]
        return pltpu.make_async_remote_copy(
            block, block, cs.at[far, k], cr.at[far, k], device_id=(e, hc), device_id_type=MESH
        )

    def from_beside(k, far):
        return pltpu.make_async_remote_copy(
            send.at[e], x.at[hxc if far else hc, partner(k)], cs.at[far, k], cr.at[far, k],
            device_id=(e, hc), device_id_type=MESH,
        )

    def give(k, far):
        return pltpu.make_async_remote_copy(
            o.at[hxc if far else hc, partner(k)], near.at[far, k], gs.at[far, k], gr.at[far, k],
            device_id=(e, hc), device_id_type=MESH,
        )

    def pair_over(k):
        return pltpu.make_async_remote_copy(
            o.at[hx, partner(k)], far_in.at[k], fs.at[k], fr.at[k], device_id=(e, hx), device_id_type=MESH
        )

    def home(k):
        return pltpu.make_async_remote_copy(
            o.at[h, partner(k)], back.at[e], hs.at[k], hr.at[k], device_id=(partner(k), h), device_id_type=MESH
        )

    def from_home(k):
        return pltpu.make_async_remote_copy(
            o.at[h, e], back.at[partner(k)], hs.at[k], hr.at[k], device_id=(partner(k), h), device_id_type=MESH
        )

    def weights(j):
        return (
            pltpu.make_async_copy(wi_hbm.at[j], wi.at[j], ws.at[0, j]),
            pltpu.make_async_copy(wo_hbm.at[j], wo.at[j], ws.at[1, j]),
        )

    for j in range(held):
        for copy in weights(j):
            copy.start()
    barrier = pltpu.get_barrier_semaphore()
    for k in range(1, owners):
        pl.semaphore_signal(barrier, inc=1, device_id=(partner(k), h), device_id_type=MESH)
    for other in (hx, hc):
        pl.semaphore_signal(barrier, inc=1, device_id=(e, other), device_id_type=MESH)

    def fill(t, carry):
        x[h, e, t] = send[e, t]
        return carry

    lax.fori_loop(0, tiles, fill, 0)
    pl.semaphore_wait(barrier, owners + 1)
    across(0).start()
    beside(0, 0).start()
    for k in masks((0,) + tuple(SEND), owners)[1:]:
        to_owner(k).start()

    flags[...] = jnp.zeros(flags.shape, f32)
    picked[...] = jnp.zeros(picked.shape, bf16)

    plan = [(min(one, two), one + in_middle * (two - one)) for one, two in zip(masks(RETURN_ENDS, owners), masks(RETURN_MIDDLE, owners))]

    def add_pair(k):
        give(k, 1).wait_recv()

        def one_tile(t, carry):
            o[hx, partner(k), t] = (o[hx, partner(k), t].astype(f32) + near[1, k, t].astype(f32)).astype(bf16)
            return carry

        lax.fori_loop(0, tiles, one_tile, 0)

    def add_all(k):
        give(k, 0).wait_recv()
        pair_over(k).wait_recv()

        def one_tile(t, carry):
            o[h, partner(k), t] = (
                o[h, partner(k), t].astype(f32) + near[0, k, t].astype(f32) + far_in[k, t].astype(f32)
            ).astype(bf16)
            return carry

        lax.fori_loop(0, tiles, one_tile, 0)

    def compute(k):
        source = partner(k)
        notes = [x[c, source, tiles - 1][TILE - 1 : TILE, :128].astype(f32) for c in range(helpers)]
        seen = flags[0:1, :]
        for note in notes:
            seen = jnp.maximum(seen, note)
        flags[0:1, :] = seen
        reached = 0
        spans = windows(held, tiles)
        for j in sorted(range(held), key=lambda j: (spans[j][0] - spans[j][1], j)):
            low, high = spans[j]
            size = (high - low) * TILE
            taken = jnp.concatenate([x[c, source, low:high].reshape(size, width) for c in range(helpers)], axis=0)
            hidden = jnp.maximum(jnp.dot(taken, wi[j], preferred_element_type=f32), 0.0).astype(bf16)
            made = jnp.dot(hidden, wo[j], preferred_element_type=f32)
            row = (lax.broadcasted_iota(jnp.int32, (size, width), 0) + low * TILE).astype(f32)
            fresh = max(low, min(reached, high))
            for c in range(helpers):
                mine = (row >= notes[c][:, j : j + 1]) & (row < notes[c][:, held + j : held + j + 1])
                own = made[c * size : (c + 1) * size]
                if fresh > low:
                    upto = (fresh - low) * TILE
                    old = o[c, source, low:fresh].reshape(upto, width).astype(f32)
                    new = jnp.where(mine[:upto], own[:upto], old).astype(bf16)
                    o[c, source, low:fresh] = new.reshape(fresh - low, TILE, width)
                if high > fresh:
                    after = (fresh - low) * TILE
                    new = jnp.where(mine[after:], own[after:], 0.0).astype(bf16)
                    o[c, source, fresh:high] = new.reshape(high - fresh, TILE, width)
            reached = max(reached, high)

    def give_both(k):
        give(k, 1).start()
        give(k, 0).start()

    def start_home(always, k):
        if always:
            home(k).start()
        else:

            @pl.when(k > 0)
            def _():
                home(k).start()

    def send_pairs(turns):
        for n, (_, k) in enumerate(turns):
            add_pair(k)
            if n:
                pair_over(turns[n - 1][1]).start()
        return turns[-1:]

    taken = masks(TAKE, owners)

    def at(i):
        k = 0
        for n, mask in enumerate(taken):
            k = k + mask * jnp.where(i == n, 1, 0)
        return k

    def forward(k):
        from_owner(k).wait_recv()
        across(k).start()
        beside(k, 0).start()

    for k in taken[1:AHEAD]:
        forward(k)
    for j in range(held):
        for copy in weights(j):
            copy.wait()

    def step(i, carry):
        k = at(i)

        @pl.when(i + AHEAD < owners)
        def _():
            forward(at(i + AHEAD))

        from_across(k).wait_recv()
        beside(k, 1).start()

        @pl.when(i > 0)
        def _():
            give_both(at(i - 1))

        for n, turns in ((owners - 2, plan[:1]), (owners - 1, plan[1:3])):

            @pl.when(i == n)
            def _(turns=turns):
                for _, late in send_pairs(turns):
                    pair_over(late).start()

        from_beside(k, 0).wait_recv()
        from_beside(k, 1).wait_recv()
        compute(k)
        return carry

    lax.fori_loop(0, owners, step, 0)
    for k in range(1, owners):
        to_owner(k).wait_send()
    give_both(taken[-1])
    late = send_pairs(plan[3:])
    add_all(plan[0][1])
    pair_over(late[0][1]).start()
    waiting = plan[0]
    for always, k in plan[1:]:
        add_all(k)
        start_home(*waiting)
        waiting = always, k
    start_home(*waiting)
    place = places[0:1, :]

    def keep(t, carry):
        back[e, t] = o[h, e, t]
        return carry

    lax.fori_loop(0, tiles, keep, 0)

    def collect(n, carry):
        hots, found = [], []
        for k in (owners - 1 - 2 * n, owners - 2 - 2 * n):
            group = partner(k)

            @pl.when(k > 0)
            def _(k=k):
                from_home(k).wait_recv()

            found.append(back[group].reshape(block, width))
            row = lax.broadcasted_iota(jnp.int32, (block, rows), 0) + group * block
            hots.append(jnp.where(row == place, 1.0, 0.0).astype(bf16))
        part = lax.dot_general(
            jnp.concatenate(hots, axis=0), jnp.concatenate(found, axis=0), (((0,), (0,)), ((), ())),
            preferred_element_type=f32,
        )
        picked[...] = (picked[...].astype(f32) + part).astype(bf16)
        return carry

    lax.fori_loop(0, owners // 2, collect, 0)
    for k in range(owners):
        across(k).wait_send()
        pair_over(k).wait_send()
        for far in (0, 1):
            beside(k, far).wait_send()
            give(k, far).wait_send()
        if k:
            home(k).wait_send()


def pack_kernel(owners, held, block, spans, first, backup, capacity, done, tokens, send, where, takes_out):
    f32, bf16, i32 = jnp.float32, jnp.bfloat16, jnp.int32
    experts, rows, width, lanes = owners * held, first.shape[1], tokens.shape[1], 128
    usable, tiles = block - 1, block // TILE
    room = capacity[...].astype(f32)
    expert = lax.broadcasted_iota(i32, (experts, rows), 0)
    earlier = (
        lax.broadcasted_iota(i32, (lanes, lanes), 0) < lax.broadcasted_iota(i32, (lanes, lanes), 1)
    ).astype(f32).astype(bf16)

    def ranks(hit):
        pieces = [hit[:, at : at + lanes] for at in range(0, rows, lanes)]
        inner = jnp.dot(jnp.concatenate(pieces, axis=0).astype(bf16), earlier, preferred_element_type=f32)
        total, out = jnp.zeros((experts, 1), f32), []
        for n, piece in enumerate(pieces):
            out.append(inner[n * experts : (n + 1) * experts] + total)
            total = total + jnp.sum(piece, axis=1, keepdims=True)
        return jnp.concatenate(out, axis=1), total

    chosen = jnp.where(expert == first[...], 1.0, 0.0)
    before, named = ranks(chosen)
    kept = jnp.where(before < room, chosen, 0.0)
    stays = jnp.max(kept, axis=0, keepdims=True)
    spill = jnp.where(expert == backup[...], 1.0 - stays, 0.0)
    spilled, extra = ranks(spill)
    kept_count = jnp.minimum(named, room)
    final = kept + spill
    rank = jnp.where(kept > 0.0, before, kept_count + spilled) - done[...]
    todo = jnp.broadcast_to(kept_count + extra - done[...], (experts, lanes))

    turn = lax.broadcasted_iota(i32, (experts, lanes), 0) % held
    same = (
        lax.broadcasted_iota(i32, (experts, experts), 0) // held == lax.broadcasted_iota(i32, (experts, experts), 1) // held
    ).astype(f32).astype(bf16)

    def group_sum(values):
        return jnp.dot(same, values.astype(bf16), preferred_element_type=f32)

    takes, starts = jnp.zeros((experts, lanes), f32), jnp.zeros((experts, lanes), f32)
    used = jnp.zeros((experts, lanes), f32)
    for j in range(held // 2):
        take = jnp.minimum(todo, min(spans[j][1] * TILE, usable) - used)
        takes = jnp.where(turn == j, take, takes)
        starts = jnp.where(turn == j, used, starts)
        used = used + group_sum(jnp.where(turn == j, take, 0.0))
    end = jnp.full((experts, lanes), float(usable), f32)
    for j in range(held - 1, held // 2 - 1, -1):
        take = jnp.minimum(jnp.minimum(todo, end - spans[j][0] * TILE), end - used)
        takes = jnp.where(turn == j, take, takes)
        starts = jnp.where(turn == j, end - take, starts)
        end = end - group_sum(jnp.where(turn == j, take, 0.0))
    takes_out[...] = takes
    left = jnp.max(todo - takes, axis=0, keepdims=True)

    here = jnp.where((rank >= 0.0) & (rank < takes[:, :1]), final, 0.0)
    base = starts[:, :1] + (lax.broadcasted_iota(i32, (experts, 1), 0) // held * block + 1).astype(f32)
    place = jnp.sum(here * (rank + base), axis=0, keepdims=True).astype(i32) - 1
    where[...] = jnp.broadcast_to(place, where.shape)

    lane = lax.broadcasted_iota(i32, (experts, lanes), 1)
    notes = jnp.where(lane == turn, starts, jnp.where(lane == held + turn, starts + takes, 0.0))
    notes = group_sum(notes)
    notes = jnp.where(lane == 2 * held, jnp.where(left > 0.0, 1.0, 0.0), notes)
    last = lax.broadcasted_iota(i32, (block, lanes), 0) == usable
    data = tokens[...]
    for group in range(owners):
        hot = jnp.where(lax.broadcasted_iota(i32, (block, rows), 0) + group * block == place, 1.0, 0.0).astype(bf16)
        packed = jnp.dot(hot, data, preferred_element_type=f32)
        note = jnp.where(last, notes[group * held : group * held + 1, :], packed[:, :lanes])
        packed = jnp.concatenate([note, packed[:, lanes:]], axis=1).astype(bf16)
        send[group] = packed.reshape(tiles, TILE, width)


def pack(owners, held, tiles, first, backup, capacity, done, tokens):
    rows, width = tokens.shape
    experts = owners * held
    return pl.pallas_call(
        functools.partial(pack_kernel, owners, held, tiles * TILE, windows(held, tiles)),
        out_shape=(
            jax.ShapeDtypeStruct((owners, tiles, TILE, width), jnp.bfloat16),
            jax.ShapeDtypeStruct((8, rows), jnp.int32),
            jax.ShapeDtypeStruct((experts, 128), jnp.float32),
        ),
        in_specs=[pl.BlockSpec(memory_space=pltpu.VMEM)] * 5,
        out_specs=[pl.BlockSpec(memory_space=pltpu.VMEM)] * 3,
        compiler_params=pltpu.CompilerParams(vmem_limit_bytes=40 * 2**20),
        name="pack",
    )(first, backup, capacity, done, tokens)


def on_device(tokens, gate, expert_ids, backup_ids, capacity, w_in, w_out):
    held = w_in.shape[0]
    owners, helpers = lax.axis_size("expert"), lax.axis_size("helper")
    rows, width = tokens.shape
    experts = held * owners
    tiles = -(-(13 * rows // (8 * owners)) // TILE)
    block = tiles * TILE
    f32, bf16 = jnp.float32, jnp.bfloat16
    dma = pltpu.SemaphoreType.DMA
    anywhere = pl.BlockSpec(memory_space=pl.ANY)
    vmem = pl.BlockSpec(memory_space=pltpu.VMEM)
    piece = (tiles, TILE, width)

    blocks = owners * piece[0] * piece[1] * width * 2
    room = blocks * (2 * helpers + 4) + 2 * w_in.size * 2 + rows * width * 2 + 12 * 2**20
    layer = pl.pallas_call(
        functools.partial(layer_kernel, owners, helpers, held),
        out_shape=(jax.ShapeDtypeStruct((rows, width), bf16), jax.ShapeDtypeStruct((8, 128), f32)),
        in_specs=[vmem, vmem, anywhere, anywhere],
        out_specs=(vmem, vmem),
        scratch_shapes=[
            pltpu.VMEM((owners,) + piece, bf16),
            pltpu.VMEM((helpers, owners) + piece, bf16),
            pltpu.VMEM((helpers, owners) + piece, bf16),
            pltpu.VMEM((2, owners) + piece, bf16),
            pltpu.VMEM((owners,) + piece, bf16),
            pltpu.VMEM(w_in.shape, bf16),
            pltpu.VMEM(w_out.shape, bf16),
            dma((owners,)), dma((owners,)), dma((owners,)), dma((owners,)),
            dma((2, owners)), dma((2, owners)), dma((2, owners)), dma((2, owners)),
            dma((owners,)), dma((owners,)), dma((owners,)), dma((owners,)),
            dma((2, held)),
        ],
        compiler_params=pltpu.CompilerParams(
            collective_id=0, has_side_effects=True, vmem_limit_bytes=min(VMEM_BYTES, room)
        ),
        name="layer",
    )

    first, backup = expert_ids.reshape(1, rows), backup_ids.reshape(1, rows)
    limits = capacity.reshape(experts, 1)

    def exchange(done):
        send, places, takes = pack(owners, held, tiles, first, backup, limits, done, tokens)
        picked, flags = layer(send, places, w_in, w_out)
        mixed = (gate[:, None] * picked.astype(f32)).astype(bf16)
        return mixed, places[0] >= 0, done + takes[:, :1], flags[0, 2 * held] > 0

    mixed, _, done, more = exchange(jnp.zeros((experts, 1), f32))

    def again(state):
        mixed, done, _ = state
        late, here, done, more = exchange(done)
        return jnp.where(here[:, None], late, mixed), done, more

    return lax.while_loop(lambda state: state[2], again, (mixed, done, more))[0]


def solution(mesh):
    placed = (
        P(("expert", "helper"), None),
        P(("expert", "helper")),
        P(("expert", "helper"), None),
        P(("expert", "helper"), None),
        P(),
        P("expert", None, "helper"),
        P("expert", "helper", None),
    )
    return jax.shard_map(
        on_device, mesh=mesh, in_specs=placed, out_specs=P(("expert", "helper"), None), check_vma=False
    )
```
